512 devices in a mesh: gx: 16 (over y_hi, z), gy: 4 (over y_lo), gz: 8 (over x, core).
Axes of the slice: x: 4, y: 8 (y_hi: 2, y_lo: 4; y = y_hi * 4 + y_lo), z: 8, core: 2. Of those that a mesh axis runs over, the one named last changes fastest.
Arguments:
- pair: bfloat16 [512, 512, 128], P('gx', ('gy', 'gz')), may hold values from -6 to 6
- pair_mask: int32 [512, 512], P('gx', ('gy', 'gz')), may hold values 0 or 1
- in_gain: float32 [128], replicated, may hold values from 0.1 to 1.9
- in_bias: float32 [128], replicated, may hold values from -3 to 3
- proj_weight: bfloat16 [128, 512], replicated, may hold values from -0.5 to 0.5
- gate_weight: bfloat16 [128, 128], replicated, may hold values from -0.5 to 0.5
- out_gain: float32 [128], replicated, may hold values from 0.1 to 1.9
- out_bias: float32 [128], replicated, may hold values from -3 to 3
- out_weight: bfloat16 [128, 128], replicated, may hold values from -0.5 to 0.5
Outputs:
- update: bfloat16 [512, 512, 128], P('gx', ('gy', 'gz'))
The draws below stay inside these ranges and needn't reach their ends.
All inputs are finite; a program needn't handle non-finite values. No bound on the sum of `pair_mask` on one device may be relied on, other than what follows from the above.
Results may differ from the reference program's by a relative error of at most 0.0071.
Values may be sent and summed in bfloat16 or wider, within the bound.
A program may use at most 64 MiB of HBM per device.

```python
import jax
import jax.numpy as jnp
from jax import lax

C = 128
CH = 128
N = 512


def with_ends(array, stream_key, smallest, high):
    spot = [jax.random.randint(jax.random.fold_in(stream_key, axis), (), 0, length) for axis, length in enumerate(array.shape)]
    widest = array.shape.index(max(array.shape))
    beside = spot[:widest] + [(spot[widest] + 1) % array.shape[widest]] + spot[widest + 1:]
    return array.at[tuple(spot)].set(smallest).at[tuple(beside)].set(high)


def block_levels(stream_key, shape, pieces, low, largest):
    loudness = 1.0
    for axis_at, parts in pieces:
        steps = jax.random.uniform(jax.random.fold_in(jax.random.fold_in(stream_key, 6), axis_at), (parts,), jnp.float32, low / len(pieces), largest / len(pieces))
        loudness = loudness * jnp.repeat(jnp.exp(steps), shape[axis_at] // parts).reshape((-1,) + (1,) * (len(shape) - 1 - axis_at))
    return loudness


def gaussian(key, shape, scale, reach, split=(), held_as=jnp.bfloat16):
    result = scale * jax.random.normal(key, shape, jnp.float32)
    if split:
        result = result * block_levels(key, shape, split, -0.22, 0.18)
    return jnp.clip(result, -reach, reach).astype(held_as)


def setup_inputs(seed: int = 0) -> dict:
    splits = jax.random.split(jax.random.key(seed), 10)
    pair = gaussian(splits[0], (N, N, C), 1.0, 6.0, ((0, 16), (1, 32)))
    pair_mask = with_ends((jax.random.randint(splits[1], (N, N), 0, 4) < 3).astype(jnp.int32), jax.random.fold_in(splits[1], 1), 0, 1)
    in_gain = jnp.clip(1.0 + 0.18 * jax.random.normal(splits[2], (C,), jnp.float32), 0.1, 1.9)
    in_bias = gaussian(splits[3], (C,), 0.5, 3.0, (), jnp.float32)
    proj_weight = gaussian(splits[4], (C, 4 * CH), C ** -0.5, 0.5)
    gate_weight = gaussian(splits[5], (C, C), C ** -0.5, 0.5)
    out_gain = jnp.clip(1.0 + 0.18 * jax.random.normal(splits[6], (CH,), jnp.float32), 0.1, 1.9)
    out_bias = gaussian(splits[7], (CH,), 0.5, 3.0, (), jnp.float32)
    out_weight = gaussian(splits[8], (CH, C), CH ** -0.5, 0.5)
    return dict(pair=pair, pair_mask=pair_mask, in_gain=in_gain, in_bias=in_bias, proj_weight=proj_weight, gate_weight=gate_weight, out_gain=out_gain, out_bias=out_bias, out_weight=out_weight)


def normalize(values, gain, bias):
    average = lax.optimization_barrier(jnp.mean(values, axis=-1, keepdims=True))
    centered = values - average
    variance = lax.optimization_barrier(jnp.mean(centered * centered, axis=-1, keepdims=True))
    return centered * lax.rsqrt(variance + 1e-05) * gain + bias

def reference(pair, pair_mask, in_gain, in_bias, proj_weight, gate_weight, out_gain, out_bias, out_weight):
    total = pair.shape[0]
    channels = pair.shape[2]
    hidden = proj_weight.shape[1] // 4
    normed = normalize(pair.astype(jnp.float32), in_gain, in_bias).astype(jnp.bfloat16)
    flat = normed.reshape(total * total, channels)
    projected = jnp.dot(flat, proj_weight, preferred_element_type=jnp.float32).reshape(total, total, 4 * hidden)
    mask_value = pair_mask.astype(jnp.float32)[:, :, None]
    left_side = (jax.nn.sigmoid(projected[:, :, :hidden]) * projected[:, :, hidden:2 * hidden] * mask_value).astype(jnp.bfloat16)
    right_side = (jax.nn.sigmoid(projected[:, :, 2 * hidden:3 * hidden]) * projected[:, :, 3 * hidden:] * mask_value).astype(jnp.bfloat16)
    triangle = jnp.einsum('ikc,jkc->ijc', left_side.astype(jnp.float32), right_side.astype(jnp.float32), precision=lax.Precision.HIGHEST)
    tri_normed = normalize(triangle, out_gain, out_bias).astype(jnp.bfloat16)
    gating = jax.nn.sigmoid(jnp.dot(flat, gate_weight, preferred_element_type=jnp.float32))
    mixed = jnp.dot(tri_normed.reshape(total * total, hidden), out_weight, preferred_element_type=jnp.float32)
    return (gating * mixed).reshape(total, total, channels).astype(jnp.bfloat16)
```

```python
import functools

import jax
import jax.numpy as jnp
from jax import lax
from jax.experimental import pallas as pl
from jax.experimental.pallas import tpu as pltpu
from jax.sharding import PartitionSpec as P

MESH = pl.DeviceIdType.MESH
F32, BF16 = jnp.float32, jnp.bfloat16
EPS = 1e-05


def dot(a, b, ca, cb):
    return lax.dot_general(a, b, (((ca,), (cb,)), ((), ())), preferred_element_type=F32)


def exchange_blocks(tiles):
    block = lax.broadcasted_iota(jnp.int32, tiles[0].shape, 1) // 32
    rolled = [[t if d == 0 else pltpu.roll(t, 32 * d, 1) for d in range(4)] for t in tiles]
    outs = []
    for b in range(4):
        out = rolled[0][(0 - b) % 4]
        for a in range(1, 4):
            out = jnp.where(block == a, rolled[a][(a - b) % 4], out)
        outs.append(out)
    return outs


def kernel(
    pair_hbm, mask_hbm, in_gain_hbm, in_bias_hbm, proj_hbm, gatew_hbm, out_gain_hbm, out_bias_hbm, outw_hbm,
    out_ref,
    pair, mask, in_gain, in_bias, proj, gatew, out_gain, out_bias, outw,
    normed, staged, send1, recv1, ops, oplane, xsend, xrecv, own, send3, tri, wide, gating, mixed,
    load_sem, s1, r1, sd, rd, sx, rx, s3, r3, se, re,
):
    gx, gy, gz = lax.axis_index("gx"), lax.axis_index("gy"), lax.axis_index("gz")
    x, core = gz // 2, gz % 2
    me = gx * 4 + gy
    partner = (gx, gy, x * 2 + 1 - core)

    def plane(p):
        return (p // 4, p % 4, gz)

    def along_x(d):
        return (gx, gy, ((x + d) % 4) * 2 + core)

    barrier = pltpu.get_barrier_semaphore()

    def greet(t, carry):
        pl.semaphore_signal(barrier, inc=1, device_id=plane((t + me) % 64), device_id_type=MESH)
        return carry

    lax.fori_loop(1, 64, greet, 0)
    for d in range(1, 4):
        pl.semaphore_signal(barrier, inc=1, device_id=along_x(d), device_id_type=MESH)
    pl.semaphore_signal(barrier, inc=1, device_id=partner, device_id_type=MESH)

    sources = (pair_hbm, mask_hbm, in_gain_hbm, in_bias_hbm, proj_hbm, gatew_hbm, out_gain_hbm, out_bias_hbm, outw_hbm)
    places = (pair, mask, in_gain, in_bias, proj, gatew, out_gain, out_bias, outw)
    loads = [pltpu.make_async_copy(s, d, load_sem.at[n]) for n, (s, d) in enumerate(zip(sources, places))]
    for load in loads:
        load.start()
    for load in loads:
        load.wait()

    tile = pair[...].astype(F32).reshape(512, 128)
    centered = tile - jnp.mean(tile, axis=-1, keepdims=True)
    variance = jnp.mean(centered * centered, axis=-1, keepdims=True)
    scaled = centered * lax.rsqrt(variance + EPS) * in_gain[...] + in_bias[...]
    normed[...] = scaled.astype(BF16).astype(F32)
    mask_value = mask[...].astype(F32)
    rows = []
    for k in range(16):
        rows.append(normed[pl.ds(k, 32, stride=16), :] * mask_value[:, k : k + 1])
    masked = jnp.concatenate(rows, axis=0).astype(BF16)
    projected = dot(jnp.transpose(proj[...]), masked, 1, 1)
    for side in range(2):
        gate = projected[256 * side : 256 * side + 128, :]
        value = projected[256 * side + 128 : 256 * side + 256, :]
        both = jax.nn.sigmoid(gate) * value
        for par in range(2):
            for q in range(4):
                staged[pl.ds(side * 8 + par * 4 + q, 64, stride=16), :] = both[
                    par * 64 : par * 64 + 64, q * 128 : q * 128 + 128
                ]
    send1[...] = staged[...].astype(BF16).reshape(64, 16, 128)

    pl.semaphore_wait(barrier, 67)

    def send_first(t, carry):
        p = (t + me) % 64
        pltpu.make_async_remote_copy(
            send1.at[p], recv1.at[me], s1, r1, device_id=plane(p), device_id_type=MESH
        ).start()
        return carry

    lax.fori_loop(1, 64, send_first, 0)
    recv1[me] = send1[me]

    gates = dot(normed[...].astype(BF16), gatew[...], 1, 0)
    gating[...] = jax.nn.sigmoid(gates).reshape(32, 16, 128)

    pltpu.make_async_copy(send1.at[pl.ds(0, 63)], send1.at[pl.ds(0, 63)], s1).wait()
    pltpu.make_async_copy(recv1.at[pl.ds(0, 63)], recv1.at[pl.ds(0, 63)], r1).wait()

    low = lax.broadcasted_iota(jnp.int32, (8, 128), 0) < 4
    for side in range(2):
        for group in range(4):
            for y in range(4):
                if side == 0:
                    members = [4 * group + a for a in range(4)]
                else:
                    members = [4 * a + group for a in range(4)]
                tiles = [recv1[m * 4 + y, side * 8 : side * 8 + 8, :].astype(F32) for m in members]
                outs = exchange_blocks(tiles)
                turned = [pltpu.roll(o, 4, 0) for o in outs]
                first = [jnp.where(low, outs[2 * h], turned[2 * h + 1]) for h in range(2)]
                second = [jnp.where(low, turned[2 * h], outs[2 * h + 1]) for h in range(2)]
                at = (pl.ds(y * 16, 16), pl.ds(group * 128, 128))
                ops[0, side, at[0], at[1]] = jnp.concatenate(first, axis=0).astype(BF16)
                ops[1, side, at[0], at[1]] = jnp.concatenate(second, axis=0).astype(BF16)

    cross = pltpu.make_async_remote_copy(
        ops.at[1 - core], oplane, sd, rd, device_id=partner, device_id_type=MESH
    )
    cross.start()
    left = [jnp.transpose(ops[core, 0])]
    cross.wait()
    left.append(jnp.transpose(oplane[0]))
    left = jnp.concatenate(left, axis=1)

    copies = []
    for d in range(1, 5):
        at = pl.ds(pl.multiple_of(((x + d) % 4) * 128, 128), 128)
        right = jnp.concatenate([ops[core, 1, :, at], oplane[1, :, at]], axis=0)
        part = dot(left, right, 1, 0)
        if d < 4:
            xsend[d - 1] = part.astype(BF16)
            copy = pltpu.make_async_remote_copy(
                xsend.at[d - 1], xrecv.at[d - 1], sx.at[d - 1], rx.at[d - 1], device_id=along_x(d), device_id_type=MESH
            )
            copy.start()
            copies.append(copy)
        else:
            own[...] = part
    for copy in copies:
        copy.wait()

    for g in range(16):
        tiles = []
        for s in range(4):
            at = pl.ds(g * 32 + s * 8, 8)
            total = own[at, :]
            for d in range(3):
                total = total + xrecv[d, at, :].astype(F32)
            tiles.append(total)
        for w, out in enumerate(exchange_blocks(tiles)):
            send3[g * 4 + w] = out.astype(BF16)

    def send_third(t, carry):
        p = (t + me) % 64
        pltpu.make_async_remote_copy(
            send3.at[p], tri.at[core, me], s3, r3, device_id=plane(p), device_id_type=MESH
        ).start()
        return carry

    lax.fori_loop(1, 64, send_third, 0)
    tri[core, me] = send3[me]
    pltpu.make_async_copy(send3.at[pl.ds(0, 63)], send3.at[pl.ds(0, 63)], s3).wait()
    pltpu.make_async_copy(send3.at[pl.ds(0, 63)], tri.at[core, pl.ds(0, 63)], r3).wait()
    swap = pltpu.make_async_remote_copy(
        tri.at[core], tri.at[core], se, re, device_id=partner, device_id_type=MESH
    )
    swap.start()
    gain = jnp.transpose(jnp.broadcast_to(out_gain[...], (128, 128)))
    bias = jnp.transpose(jnp.broadcast_to(out_bias[...], (128, 128)))
    swap.wait()

    wide[...] = tri[...].astype(F32).reshape(1024, 128)
    for r in range(8):
        sums = wide[pl.ds(r, 128, stride=8), :]
        off = sums - jnp.mean(sums, axis=0, keepdims=True)
        spread = jnp.mean(off * off, axis=0, keepdims=True)
        tri_normed = (off * lax.rsqrt(spread + EPS) * gain + bias).astype(BF16)
        mixed[r] = dot(jnp.transpose(tri_normed), outw[...], 1, 0).reshape(4, 2, 16, 128)
    for r in range(8):
        for s in range(4):
            out_ref[s * 8 + r] = (gating[s * 8 + r] * mixed[r, s, core]).astype(BF16)


def on_device(pair, pair_mask, in_gain, in_bias, proj_weight, gate_weight, out_gain, out_bias, out_weight):
    vmem = pltpu.VMEM
    dma = pltpu.SemaphoreType.DMA
    args = (
        pair, pair_mask, in_gain.reshape(1, 128), in_bias.reshape(1, 128), proj_weight, gate_weight,
        out_gain.reshape(1, 128), out_bias.reshape(1, 128), out_weight,
    )
    return pl.pallas_call(
        kernel,
        out_shape=jax.ShapeDtypeStruct((32, 16, 128), BF16),
        in_specs=[pl.BlockSpec(memory_space=pl.ANY)] * 9,
        out_specs=pl.BlockSpec(memory_space=pltpu.VMEM),
        scratch_shapes=[vmem(a.shape, a.dtype) for a in args]
        + [
            vmem((512, 128), F32),
            vmem((1024, 128), F32),
            vmem((64, 16, 128), BF16),
            vmem((64, 16, 128), BF16),
            vmem((2, 2, 64, 512), BF16),
            vmem((2, 64, 512), BF16),
            vmem((3, 512, 128), BF16),
            vmem((3, 512, 128), BF16),
            vmem((512, 128), F32),
            vmem((64, 8, 128), BF16),
            vmem((2, 64, 8, 128), BF16),
            vmem((1024, 128), F32),
            vmem((32, 16, 128), F32),
            vmem((8, 4, 2, 16, 128), F32),
            dma((9,)), dma, dma, dma, dma, dma((3,)), dma((3,)), dma, dma, dma, dma,
        ],
        compiler_params=pltpu.CompilerParams(collective_id=1, has_side_effects=True),
    )(*args)


def solution(mesh):
    rows = P("gx", ("gy", "gz"), None)
    in_specs = (rows, P("gx", ("gy", "gz")), P(), P(), P(), P(), P(), P(), P())
    return jax.shard_map(on_device, mesh=mesh, in_specs=in_specs, out_specs=rows, check_vma=False)
```

```python
import jax
import jax.numpy as jnp
from jax import lax
from jax.experimental import pallas as pl
from jax.experimental.pallas import tpu as pltpu
from jax.sharding import PartitionSpec as P

MESH = pl.DeviceIdType.MESH
F32, BF16 = jnp.float32, jnp.bfloat16
EPS = 1e-05


def dot(a, b, ca, cb):
    return lax.dot_general(a, b, (((ca,), (cb,)), ((), ())), preferred_element_type=F32)


def lanes(shape):
    return lax.broadcasted_iota(jnp.int32, shape, 1)


def exchange_blocks(tiles):
    block = lanes(tiles[0].shape) // 32
    rolled = [[t if d == 0 else pltpu.roll(t, 32 * d, 1) for d in range(4)] for t in tiles]
    outs = []
    for b in range(4):
        out = rolled[0][(0 - b) % 4]
        for a in range(1, 4):
            out = jnp.where(block == a, rolled[a][(a - b) % 4], out)
        outs.append(out)
    return outs


def kernel(
    pair_hbm, mask_hbm, in_gain_hbm, in_bias_hbm, proj_hbm, gatew_hbm, out_gain_hbm, out_bias_hbm, outw_hbm,
    out_ref,
    pair, mask, in_gain, in_bias, proj, gatew, out_gain, out_bias, outw,
    normed, staged, send1, recv1, left, left_in, right, right_in, rows, xsend, xrecv, own, send3, tri, wide,
    gating, mixed,
    load_sem, s1, r1, sl, rl, sr, rr, sx, rx, s3, r3,
):
    gx, gy, gz = lax.axis_index("gx"), lax.axis_index("gy"), lax.axis_index("gz")
    x, core = gz // 2, gz % 2
    me = gx * 4 + gy
    partner = (gx, gy, x * 2 + 1 - core)

    def plane(p):
        return (p // 4, p % 4, gz)

    def along_x(d):
        return (gx, gy, ((x + d) % 4) * 2 + core)

    barrier = pltpu.get_barrier_semaphore()

    def greet(t, carry):
        pl.semaphore_signal(barrier, inc=1, device_id=plane((t + me) % 64), device_id_type=MESH)
        return carry

    lax.fori_loop(1, 64, greet, 0)
    for d in range(1, 4):
        pl.semaphore_signal(barrier, inc=1, device_id=along_x(d), device_id_type=MESH)
    pl.semaphore_signal(barrier, inc=1, device_id=partner, device_id_type=MESH)

    sources = (pair_hbm, mask_hbm, in_gain_hbm, in_bias_hbm, proj_hbm, gatew_hbm, out_gain_hbm, out_bias_hbm, outw_hbm)
    places = (pair, mask, in_gain, in_bias, proj, gatew, out_gain, out_bias, outw)
    loads = [pltpu.make_async_copy(s, d, load_sem.at[n]) for n, (s, d) in enumerate(zip(sources, places))]
    for load in loads:
        load.start()
    for load in loads:
        load.wait()

    tile = pair[...].astype(F32).reshape(512, 128)
    centered = tile - jnp.mean(tile, axis=-1, keepdims=True)
    variance = jnp.mean(centered * centered, axis=-1, keepdims=True)
    scaled = centered * lax.rsqrt(variance + EPS) * in_gain[...] + in_bias[...]
    normed[...] = scaled.astype(BF16).astype(F32)
    mask_value = jnp.transpose(mask[...].astype(F32))
    masked = []
    for k in range(16):
        masked.append(normed[pl.ds(k, 32, stride=16), :] * mask_value[:, k : k + 1])
    masked = jnp.concatenate(masked, axis=0).astype(BF16)
    projected = dot(jnp.transpose(proj[...]), masked, 1, 1)
    for side in range(2):
        gate = projected[256 * side : 256 * side + 128, :]
        value = projected[256 * side + 128 : 256 * side + 256, :]
        both = jax.nn.sigmoid(gate) * value
        for ch in range(2):
            for q in range(4):
                staged[ch, pl.ds(side * 4 + q, 64, stride=8), :] = both[
                    ch * 64 : ch * 64 + 64, q * 128 : q * 128 + 128
                ]
    for ch in range(2):
        send1[ch] = staged[ch].reshape(64, 8, 128).astype(BF16)

    pl.semaphore_wait(barrier, 67)

    for ch in range(2):

        def send_first(t, carry, ch=ch):
            p = (t + me) % 64
            pltpu.make_async_remote_copy(
                send1.at[ch, p], recv1.at[ch, me], s1.at[ch], r1.at[ch], device_id=plane(p), device_id_type=MESH
            ).start()
            return carry

        lax.fori_loop(1, 64, send_first, 0)
        recv1[ch, me] = send1[ch, me]

    gates = dot(normed[...].astype(BF16), gatew[...], 1, 0)
    gating[...] = jax.nn.sigmoid(gates)

    low = lax.broadcasted_iota(jnp.int32, (8, 128), 0) < 4
    near = lanes((8, 128)) % 32 < 16
    for ch in range(2):
        pltpu.make_async_copy(recv1.at[ch, pl.ds(0, 63)], recv1.at[ch, pl.ds(0, 63)], r1.at[ch]).wait()
        for pairing in range(2):
            at = [pl.ds(pairing * 32 + h * 16, 16) for h in range(2)]
            sides = [[], []]
            for g in range(16):
                one = recv1[ch, g * 4 + pairing * 2].astype(F32)
                two = recv1[ch, g * 4 + pairing * 2 + 1].astype(F32)
                sides[0].append(jnp.where(low, one, pltpu.roll(two, 4, 0)))
                sides[1].append(jnp.where(low, pltpu.roll(one, 4, 0), two))
            for group in range(4):
                outs = exchange_blocks([sides[0][4 * group + a] for a in range(4)])
                for h in range(2):
                    left[ch, at[h], pl.ds(group * 128, 128)] = jnp.concatenate(
                        [outs[2 * h], outs[2 * h + 1]], axis=0
                    ).astype(BF16)
            for xpair in range(2):
                both = [exchange_blocks([sides[1][4 * a + 2 * xpair + b] for a in range(4)]) for b in range(2)]
                for h in range(2):
                    halves = [[], []]
                    for kk in (2 * h, 2 * h + 1):
                        halves[0].append(jnp.where(near, both[0][kk], pltpu.roll(both[1][kk], 16, 1)))
                        halves[1].append(jnp.where(near, pltpu.roll(both[0][kk], 112, 1), both[1][kk]))
                    for c in range(2):
                        right[ch, c, at[h], pl.ds(xpair * 128, 128)] = jnp.concatenate(
                            halves[c], axis=0
                        ).astype(BF16)

        cross_left = pltpu.make_async_remote_copy(
            left.at[ch], left_in.at[ch], sl.at[ch], rl.at[ch], device_id=partner, device_id_type=MESH
        )
        cross_left.start()
        cross_right = pltpu.make_async_remote_copy(
            right.at[ch, 1 - core], right_in.at[ch], sr.at[ch], rr.at[ch], device_id=partner, device_id_type=MESH
        )
        cross_right.start()
        cross_left.wait()
        cross_right.wait()
        both = jnp.concatenate([right[ch, core], right_in[ch]], axis=0)
        turned = jnp.transpose(both)
        for xx in range(4):
            for v in range(4):
                at = ((xx // 2 * 4 + v) * 2 + xx % 2) * 16
                rows[xx, v * 16 : v * 16 + 16, :] = turned[at : at + 16, :]
        stacked = jnp.concatenate([left[ch], left_in[ch]], axis=0)
        for d in (2, 1, 3, 4):
            part = dot(rows[(x + d) % 4], stacked, 1, 0)
            for q in range(4):
                if d < 4:
                    xsend[ch, d - 1, q] = part[:, q * 128 : q * 128 + 128].astype(BF16)
                else:
                    own[ch, q] = part[:, q * 128 : q * 128 + 128]
            if d < 4:
                for t in range(4):
                    q = (gx // 4 + 3 - t) % 4
                    pltpu.make_async_remote_copy(
                        xsend.at[ch, d - 1, q], xrecv.at[ch, d - 1, q], sx.at[ch, d - 1, t], rx.at[ch, d - 1, t],
                        device_id=along_x(d), device_id_type=MESH,
                    ).start()

    for t in range(4):
        q = (gx // 4 + 3 - t) % 4
        totals = []
        for ch in range(2):
            for d in range(3):
                pltpu.make_async_copy(xrecv.at[ch, d, q], xrecv.at[ch, d, q], rx.at[ch, d, t]).wait()
            total = own[ch, q]
            for d in range(3):
                total = total + xrecv[ch, d, q].astype(F32)
            totals.append(total)
        for v in range(4):
            tiles = [totals[ch][v * 16 + s * 8 : v * 16 + s * 8 + 8, :] for ch in range(2) for s in range(2)]
            for g, out in enumerate(exchange_blocks(tiles)):
                send3[q, g * 4 + v] = out.astype(BF16)

        def send_third(n, carry, q=q):
            p = q * 16 + n

            @pl.when(p != me)
            def _():
                pltpu.make_async_remote_copy(
                    send3.at[q, n], tri.at[me], s3, r3, device_id=plane(p), device_id_type=MESH
                ).start()

            return carry

        lax.fori_loop(0, 16, send_third, 0)
    tri[me] = send3[gx // 4, me % 16]

    gain = jnp.transpose(jnp.broadcast_to(out_gain[...], (128, 128)))
    bias = jnp.transpose(jnp.broadcast_to(out_bias[...], (128, 128)))
    for ch in range(2):
        pltpu.make_async_copy(send1.at[ch, pl.ds(0, 63)], send1.at[ch, pl.ds(0, 63)], s1.at[ch]).wait()
        for d in range(3):
            for t in range(4):
                pltpu.make_async_copy(xsend.at[ch, d, t], xsend.at[ch, d, t], sx.at[ch, d, t]).wait()
    pltpu.make_async_copy(tri.at[pl.ds(0, 63)], tri.at[pl.ds(0, 63)], r3).wait()

    wide[...] = tri[...].astype(F32).reshape(512, 128)
    first = lanes((64, 128)) < 64
    for m in range(4):
        one = wide[pl.ds(2 * m, 64, stride=8), :]
        two = wide[pl.ds(2 * m + 1, 64, stride=8), :]
        sums = jnp.concatenate(
            [jnp.where(first, one, pltpu.roll(two, 64, 1)), jnp.where(first, pltpu.roll(one, 64, 1), two)], axis=0
        )
        off = sums - jnp.mean(sums, axis=0, keepdims=True)
        spread = jnp.mean(off * off, axis=0, keepdims=True)
        tri_normed = (off * lax.rsqrt(spread + EPS) * gain + bias).astype(BF16)
        result = dot(jnp.transpose(tri_normed), outw[...], 1, 0)
        for r in range(2):
            for s in range(2):
                at = (r * 2 + s) * 32
                mixed[pl.ds(s * 8 + 2 * m + r, 32, stride=16), :] = result[at : at + 32, :]
    out_ref[...] = (gating[...] * mixed[...]).astype(BF16).reshape(32, 16, 128)
    pltpu.make_async_copy(tri.at[pl.ds(0, 63)], tri.at[pl.ds(0, 63)], s3).wait()


def on_device(pair, pair_mask, in_gain, in_bias, proj_weight, gate_weight, out_gain, out_bias, out_weight):
    vmem = pltpu.VMEM
    dma = pltpu.SemaphoreType.DMA
    args = (
        pair, pair_mask.T, in_gain.reshape(1, 128), in_bias.reshape(1, 128), proj_weight, gate_weight,
        out_gain.reshape(1, 128), out_bias.reshape(1, 128), out_weight,
    )
    return pl.pallas_call(
        kernel,
        out_shape=jax.ShapeDtypeStruct((32, 16, 128), BF16),
        in_specs=[pl.BlockSpec(memory_space=pl.ANY)] * 9,
        out_specs=pl.BlockSpec(memory_space=pltpu.VMEM),
        scratch_shapes=[vmem(a.shape, a.dtype) for a in args]
        + [
            vmem((512, 128), F32),
            vmem((2, 512, 128), F32),
            vmem((2, 64, 8, 128), BF16),
            vmem((2, 64, 8, 128), BF16),
            vmem((2, 64, 512), BF16),
            vmem((2, 64, 512), BF16),
            vmem((2, 2, 64, 256), BF16),
            vmem((2, 64, 256), BF16),
            vmem((4, 64, 128), BF16),
            vmem((2, 3, 4, 64, 128), BF16),
            vmem((2, 3, 4, 64, 128), BF16),
            vmem((2, 4, 64, 128), F32),
            vmem((4, 16, 8, 128), BF16),
            vmem((64, 8, 128), BF16),
            vmem((512, 128), F32),
            vmem((512, 128), F32),
            vmem((512, 128), F32),
            dma((9,)), dma((2,)), dma((2,)), dma((2,)), dma((2,)), dma((2,)), dma((2,)),
            dma((2, 3, 4)), dma((2, 3, 4)), dma, dma,
        ],
        compiler_params=pltpu.CompilerParams(collective_id=1, has_side_effects=True),
    )(*args)


def solution(mesh):
    rows = P("gx", ("gy", "gz"), None)
    in_specs = (rows, P("gx", ("gy", "gz")), P(), P(), P(), P(), P(), P(), P())
    return jax.shard_map(on_device, mesh=mesh, in_specs=in_specs, out_specs=rows, check_vma=False)
```

```python
import jax
import jax.numpy as jnp
from jax import lax
from jax.experimental import pallas as pl
from jax.experimental.pallas import tpu as pltpu
from jax.sharding import PartitionSpec as P

MESH = pl.DeviceIdType.MESH
F32, BF16 = jnp.float32, jnp.bfloat16
EPS = 1e-05


CHUNKS = (0, 2, 1, 3)


def around(d):
    return min(d, 8 - d)


STEPS = sorted(
    [(a, b) for a in range(8) for b in range(8) if a or b], key=lambda s: -around(s[0]) - around(s[1])
)


def dot(a, b, ca, cb):
    return lax.dot_general(a, b, (((ca,), (cb,)), ((), ())), preferred_element_type=F32)


def lanes(shape):
    return lax.broadcasted_iota(jnp.int32, shape, 1)


def exchange_blocks(tiles):
    block = lanes(tiles[0].shape) // 32
    rolled = [[t if d == 0 else pltpu.roll(t, 32 * d, 1) for d in range(4)] for t in tiles]
    outs = []
    for b in range(4):
        out = rolled[0][(0 - b) % 4]
        for a in range(1, 4):
            out = jnp.where(block == a, rolled[a][(a - b) % 4], out)
        outs.append(out)
    return outs


def kernel(
    pair_hbm, mask_hbm, in_gain_hbm, in_bias_hbm, proj_hbm, gatew_hbm, out_gain_hbm, out_bias_hbm, outw_hbm,
    out_ref,
    pair, mask, in_gain, in_bias, proj, gatew, out_gain, out_bias, outw,
    normed, staged, send1, recv1, left, left_in, right, right_in, rows, xsend, xrecv, own, send3, tri, wide,
    gating, mixed,
    load_sem, s1, r1, sl, rl, sr, rr, sx, rx, s3, r3,
):
    gx, gy, gz = lax.axis_index("gx"), lax.axis_index("gy"), lax.axis_index("gz")
    x, core = gz // 2, gz % 2
    me = gx * 4 + gy
    partner = (gx, gy, x * 2 + 1 - core)

    y = gx // 8 * 4 + gy
    zs = [(gx + d) % 8 for d in range(8)]
    ys = [(y + d) % 8 for d in range(8)]
    tops, lows = [v // 4 * 8 for v in ys], [v % 4 for v in ys]

    def plane(p):
        return (p // 4, p % 4, gz)

    others = [(tops[b] + zs[a], lows[b]) for a, b in STEPS]

    def along_x(d):
        return (gx, gy, ((x + d) % 4) * 2 + core)

    barrier = pltpu.get_barrier_semaphore()

    for g, w in others:
        pl.semaphore_signal(barrier, inc=1, device_id=(g, w, gz), device_id_type=MESH)
    for d in range(1, 4):
        pl.semaphore_signal(barrier, inc=1, device_id=along_x(d), device_id_type=MESH)
    pl.semaphore_signal(barrier, inc=1, device_id=partner, device_id_type=MESH)

    sources = (pair_hbm, mask_hbm, in_gain_hbm, in_bias_hbm, proj_hbm, gatew_hbm, out_gain_hbm, out_bias_hbm, outw_hbm)
    places = (pair, mask, in_gain, in_bias, proj, gatew, out_gain, out_bias, outw)
    loads = [pltpu.make_async_copy(s, d, load_sem.at[n]) for n, (s, d) in enumerate(zip(sources, places))]
    for load in loads:
        load.start()
    for load in loads:
        load.wait()

    tile = pair[...].astype(F32).reshape(512, 128)
    centered = tile - jnp.mean(tile, axis=-1, keepdims=True)
    variance = jnp.mean(centered * centered, axis=-1, keepdims=True)
    scaled = centered * lax.rsqrt(variance + EPS) * in_gain[...] + in_bias[...]
    normed[...] = scaled.astype(BF16).astype(F32)
    mask_value = jnp.transpose(mask[...].astype(F32))
    masked = []
    for k in range(16):
        masked.append(normed[pl.ds(k, 32, stride=16), :] * mask_value[:, k : k + 1])
    masked = jnp.concatenate(masked, axis=0).astype(BF16)
    projected = dot(jnp.transpose(proj[...]), masked, 1, 1)
    for side in range(2):
        gate = projected[256 * side : 256 * side + 128, :]
        value = projected[256 * side + 128 : 256 * side + 256, :]
        both = jax.nn.sigmoid(gate) * value
        for ch in range(2):
            for q in range(4):
                staged[ch, pl.ds(side * 4 + q, 64, stride=8), :] = both[
                    ch * 64 : ch * 64 + 64, q * 128 : q * 128 + 128
                ]
    for ch in range(2):
        send1[ch] = staged[ch].reshape(64, 8, 128).astype(BF16)

    pl.semaphore_wait(barrier, 67)

    for ch in range(2):
        for g, w in others:
            pltpu.make_async_remote_copy(
                send1.at[ch, g * 4 + w], recv1.at[ch, me], s1.at[ch], r1.at[ch], device_id=(g, w, gz),
                device_id_type=MESH,
            ).start()
        recv1[ch, me] = send1[ch, me]

    gates = dot(normed[...].astype(BF16), gatew[...], 1, 0)
    gating[...] = jax.nn.sigmoid(gates)

    low = lax.broadcasted_iota(jnp.int32, (8, 128), 0) < 4
    near = lanes((8, 128)) % 32 < 16
    for ch in range(2):
        pltpu.make_async_copy(recv1.at[ch, pl.ds(0, 63)], recv1.at[ch, pl.ds(0, 63)], r1.at[ch]).wait()
        for pairing in range(2):
            at = [pl.ds(pairing * 32 + h * 16, 16) for h in range(2)]
            sides = [[], []]
            for g in range(16):
                one = recv1[ch, g * 4 + pairing * 2].astype(F32)
                two = recv1[ch, g * 4 + pairing * 2 + 1].astype(F32)
                sides[0].append(jnp.where(low, one, pltpu.roll(two, 4, 0)))
                sides[1].append(jnp.where(low, pltpu.roll(one, 4, 0), two))
            for group in range(4):
                outs = exchange_blocks([sides[0][4 * group + a] for a in range(4)])
                for h in range(2):
                    left[ch, at[h], pl.ds(group * 128, 128)] = jnp.concatenate(
                        [outs[2 * h], outs[2 * h + 1]], axis=0
                    ).astype(BF16)
            for xpair in range(2):
                both = [exchange_blocks([sides[1][4 * a + 2 * xpair + b] for a in range(4)]) for b in range(2)]
                for h in range(2):
                    halves = [[], []]
                    for kk in (2 * h, 2 * h + 1):
                        halves[0].append(jnp.where(near, both[0][kk], pltpu.roll(both[1][kk], 16, 1)))
                        halves[1].append(jnp.where(near, pltpu.roll(both[0][kk], 112, 1), both[1][kk]))
                    for c in range(2):
                        right[ch, c, at[h], pl.ds(xpair * 128, 128)] = jnp.concatenate(
                            halves[c], axis=0
                        ).astype(BF16)

        cross_left = pltpu.make_async_remote_copy(
            left.at[ch], left_in.at[ch], sl.at[ch], rl.at[ch], device_id=partner, device_id_type=MESH
        )
        cross_left.start()
        cross_right = pltpu.make_async_remote_copy(
            right.at[ch, 1 - core], right_in.at[ch], sr.at[ch], rr.at[ch], device_id=partner, device_id_type=MESH
        )
        cross_right.start()
        cross_left.wait()
        cross_right.wait()
        both = jnp.concatenate([right[ch, core], right_in[ch]], axis=0)
        turned = jnp.transpose(both)
        for xx in range(4):
            for v in range(4):
                at = ((xx // 2 * 4 + v) * 2 + xx % 2) * 16
                rows[xx, v * 16 : v * 16 + 16, :] = turned[at : at + 16, :]
        stacked = jnp.concatenate([left[ch], left_in[ch]], axis=0)
        for d in (2, 1, 3, 4):
            part = dot(rows[(x + d) % 4], stacked, 1, 0)
            for q in range(4):
                if d < 4:
                    xsend[ch, d - 1, q] = part[:, q * 128 : q * 128 + 128].astype(BF16)
                else:
                    own[ch, q] = part[:, q * 128 : q * 128 + 128]
            if d < 4:
                for t, q in enumerate(CHUNKS):
                    pltpu.make_async_remote_copy(
                        xsend.at[ch, d - 1, q], xrecv.at[ch, d - 1, q], sx.at[ch, d - 1, t], rx.at[ch, d - 1, t],
                        device_id=along_x(d), device_id_type=MESH,
                    ).start()

    for t, q in enumerate(CHUNKS):
        totals = []
        for ch in range(2):
            for d in range(3):
                pltpu.make_async_copy(xrecv.at[ch, d, q], xrecv.at[ch, d, q], rx.at[ch, d, t]).wait()
            total = own[ch, q]
            for d in range(3):
                total = total + xrecv[ch, d, q].astype(F32)
            totals.append(total)
        for v in range(4):
            tiles = [totals[ch][v * 16 + s * 8 : v * 16 + s * 8 + 8, :] for ch in range(2) for s in range(2)]
            for g, out in enumerate(exchange_blocks(tiles)):
                send3[q, g * 4 + v] = out.astype(BF16)

        for n in range(16):
            p = q * 16 + n

            @pl.when(p != me)
            def _(n=n, p=p):
                pltpu.make_async_remote_copy(
                    send3.at[q, n], tri.at[me], s3, r3, device_id=plane(p), device_id_type=MESH
                ).start()

    tri[me] = send3[gx // 4, me % 16]

    gain = jnp.transpose(jnp.broadcast_to(out_gain[...], (128, 128)))
    bias = jnp.transpose(jnp.broadcast_to(out_bias[...], (128, 128)))
    for ch in range(2):
        pltpu.make_async_copy(send1.at[ch, pl.ds(0, 63)], send1.at[ch, pl.ds(0, 63)], s1.at[ch]).wait()
        for d in range(3):
            for t in range(4):
                pltpu.make_async_copy(xsend.at[ch, d, t], xsend.at[ch, d, t], sx.at[ch, d, t]).wait()
    pltpu.make_async_copy(tri.at[pl.ds(0, 63)], tri.at[pl.ds(0, 63)], r3).wait()

    wide[...] = tri[...].astype(F32).reshape(512, 128)
    first = lanes((64, 128)) < 64
    pieces = []
    for m in range(4):
        one = wide[pl.ds(2 * m, 64, stride=8), :]
        two = wide[pl.ds(2 * m + 1, 64, stride=8), :]
        pieces.append(
            jnp.concatenate(
                [jnp.where(first, one, pltpu.roll(two, 64, 1)), jnp.where(first, pltpu.roll(one, 64, 1), two)], axis=0
            )
        )
    sums = jnp.concatenate(pieces, axis=1)
    off = sums - jnp.mean(sums, axis=0, keepdims=True)
    spread = jnp.mean(off * off, axis=0, keepdims=True)
    scaled = off * lax.rsqrt(spread + EPS)
    tri_normed = jnp.concatenate([scaled[:, m * 128 : m * 128 + 128] * gain + bias for m in range(4)], axis=1)
    result = dot(jnp.transpose(tri_normed.astype(BF16)), outw[...], 1, 0)
    for m in range(4):
        for r in range(2):
            for s in range(2):
                at = m * 128 + (r * 2 + s) * 32
                mixed[pl.ds(s * 8 + 2 * m + r, 32, stride=16), :] = result[at : at + 32, :]
    out_ref[...] = (gating[...] * mixed[...]).astype(BF16).reshape(32, 16, 128)
    pltpu.make_async_copy(tri.at[pl.ds(0, 63)], tri.at[pl.ds(0, 63)], s3).wait()


def on_device(pair, pair_mask, in_gain, in_bias, proj_weight, gate_weight, out_gain, out_bias, out_weight):
    vmem = pltpu.VMEM
    dma = pltpu.SemaphoreType.DMA
    args = (
        pair, pair_mask.T, in_gain.reshape(1, 128), in_bias.reshape(1, 128), proj_weight, gate_weight,
        out_gain.reshape(1, 128), out_bias.reshape(1, 128), out_weight,
    )
    return pl.pallas_call(
        kernel,
        out_shape=jax.ShapeDtypeStruct((32, 16, 128), BF16),
        in_specs=[pl.BlockSpec(memory_space=pltpu.HBM)] * 9,
        out_specs=pl.BlockSpec(memory_space=pltpu.VMEM),
        scratch_shapes=[vmem(a.shape, a.dtype) for a in args]
        + [
            vmem((512, 128), F32),
            vmem((2, 512, 128), F32),
            vmem((2, 64, 8, 128), BF16),
            vmem((2, 64, 8, 128), BF16),
            vmem((2, 64, 512), BF16),
            vmem((2, 64, 512), BF16),
            vmem((2, 2, 64, 256), BF16),
            vmem((2, 64, 256), BF16),
            vmem((4, 64, 128), BF16),
            vmem((2, 3, 4, 64, 128), BF16),
            vmem((2, 3, 4, 64, 128), BF16),
            vmem((2, 4, 64, 128), F32),
            vmem((4, 16, 8, 128), BF16),
            vmem((64, 8, 128), BF16),
            vmem((512, 128), F32),
            vmem((512, 128), F32),
            vmem((512, 128), F32),
            dma((9,)), dma((2,)), dma((2,)), dma((2,)), dma((2,)), dma((2,)), dma((2,)),
            dma((2, 3, 4)), dma((2, 3, 4)), dma, dma,
        ],
        compiler_params=pltpu.CompilerParams(collective_id=1, has_side_effects=True),
    )(*args)


def solution(mesh):
    rows = P("gx", ("gy", "gz"), None)
    in_specs = (rows, P("gx", ("gy", "gz")), P(), P(), P(), P(), P(), P(), P())
    return jax.shard_map(on_device, mesh=mesh, in_specs=in_specs, out_specs=rows, check_vma=False)
```

```python
import jax
import jax.numpy as jnp
from jax import lax
from jax.experimental import pallas as pl
from jax.experimental.pallas import tpu as pltpu
from jax.sharding import PartitionSpec as P

MESH = pl.DeviceIdType.MESH
F32, BF16 = jnp.float32, jnp.bfloat16
EPS = 1e-05


CHUNKS = (0, 2, 1, 3)


def around(d):
    return min(d, 8 - d)


STEPS = sorted(
    [(a, b) for a in range(8) for b in range(8) if a or b], key=lambda s: -around(s[0]) - around(s[1])
)


def dot(a, b, ca, cb):
    return lax.dot_general(a, b, (((ca,), (cb,)), ((), ())), preferred_element_type=F32)


def lanes(shape):
    return lax.broadcasted_iota(jnp.int32, shape, 1)


def exchange_blocks(tiles):
    block = lanes(tiles[0].shape) // 32
    rolled = [[t if d == 0 else pltpu.roll(t, 32 * d, 1) for d in range(4)] for t in tiles]
    outs = []
    for b in range(4):
        out = rolled[0][(0 - b) % 4]
        for a in range(1, 4):
            out = jnp.where(block == a, rolled[a][(a - b) % 4], out)
        outs.append(out)
    return outs


def kernel(
    pair_hbm, mask_hbm, in_gain_hbm, in_bias_hbm, proj_hbm, gatew_hbm, out_gain_hbm, out_bias_hbm, outw_hbm,
    out_ref,
    pair, mask, in_gain, in_bias, proj, gatew, out_gain, out_bias, outw,
    normed, staged, send1, recv1, left, left_in, right, right_in, rows, xsend, xrecv, own, send3, tri, wide,
    gating, mixed,
    load_sem, s1, r1, sl, rl, sr, rr, sx, rx, s3, r3,
):
    gx, gy, gz = lax.axis_index("gx"), lax.axis_index("gy"), lax.axis_index("gz")
    x, core = gz // 2, gz % 2
    me = gx * 4 + gy
    partner = (gx, gy, x * 2 + 1 - core)

    y = gx // 8 * 4 + gy
    zs = [(gx + d) % 8 for d in range(8)]
    ys = [(y + d) % 8 for d in range(8)]
    tops, lows = [v // 4 * 8 for v in ys], [v % 4 for v in ys]

    def plane(p):
        return (p // 4, p % 4, gz)

    others = [(tops[b] + zs[a], lows[b]) for a, b in STEPS]

    def along_x(d):
        return (gx, gy, ((x + d) % 4) * 2 + core)

    barrier = pltpu.get_barrier_semaphore()

    for g, w in others:
        pl.semaphore_signal(barrier, inc=1, device_id=(g, w, gz), device_id_type=MESH)
    for d in range(1, 4):
        pl.semaphore_signal(barrier, inc=1, device_id=along_x(d), device_id_type=MESH)
    pl.semaphore_signal(barrier, inc=1, device_id=partner, device_id_type=MESH)

    sources = (pair_hbm, mask_hbm, in_gain_hbm, in_bias_hbm, proj_hbm, gatew_hbm, out_gain_hbm, out_bias_hbm, outw_hbm)
    places = (pair, mask, in_gain, in_bias, proj, gatew, out_gain, out_bias, outw)
    loads = [pltpu.make_async_copy(s, d, load_sem.at[n]) for n, (s, d) in enumerate(zip(sources, places))]
    for load in loads:
        load.start()
    for load in loads:
        load.wait()

    tile = pair[...].astype(F32).reshape(512, 128)
    centered = tile - jnp.mean(tile, axis=-1, keepdims=True)
    variance = jnp.mean(centered * centered, axis=-1, keepdims=True)
    scaled = centered * lax.rsqrt(variance + EPS) * in_gain[...] + in_bias[...]
    normed[...] = scaled.astype(BF16).astype(F32)
    mask_value = jnp.transpose(mask[...].astype(F32))
    masked = []
    for k in range(16):
        masked.append(normed[pl.ds(k, 32, stride=16), :] * mask_value[:, k : k + 1])
    masked = jnp.concatenate(masked, axis=0).astype(BF16)
    projected = dot(jnp.transpose(proj[...]), masked, 1, 1)
    for side in range(2):
        gate = projected[256 * side : 256 * side + 128, :]
        value = projected[256 * side + 128 : 256 * side + 256, :]
        both = jax.nn.sigmoid(gate) * value
        for ch in range(2):
            for q in range(4):
                staged[ch, pl.ds(side * 4 + q, 64, stride=8), :] = both[
                    ch * 64 : ch * 64 + 64, q * 128 : q * 128 + 128
                ]
    for ch in range(2):
        send1[ch] = staged[ch].reshape(64, 8, 128).astype(BF16)

    pl.semaphore_wait(barrier, 67)

    for ch in range(2):
        for g, w in others:
            pltpu.make_async_remote_copy(
                send1.at[ch, g * 4 + w], recv1.at[ch, me], s1.at[ch], r1.at[ch], device_id=(g, w, gz),
                device_id_type=MESH,
            ).start()
        recv1[ch, me] = send1[ch, me]

    gates = dot(normed[...].astype(BF16), gatew[...], 1, 0)
    gating[...] = jax.nn.sigmoid(gates)

    low = lax.broadcasted_iota(jnp.int32, (8, 128), 0) < 4
    near = lanes((8, 128)) % 32 < 16
    for ch in range(2):
        pltpu.make_async_copy(recv1.at[ch, pl.ds(0, 63)], recv1.at[ch, pl.ds(0, 63)], r1.at[ch]).wait()
        for pairing in range(2):
            at = [pl.ds(pairing * 32 + h * 16, 16) for h in range(2)]
            sides = [[], []]
            for g in range(16):
                one = recv1[ch, g * 4 + pairing * 2].astype(F32)
                two = recv1[ch, g * 4 + pairing * 2 + 1].astype(F32)
                sides[0].append(jnp.where(low, one, pltpu.roll(two, 4, 0)))
                sides[1].append(jnp.where(low, pltpu.roll(one, 4, 0), two))
            for group in range(4):
                outs = exchange_blocks([sides[0][4 * group + a] for a in range(4)])
                for h in range(2):
                    left[ch, at[h], pl.ds(group * 128, 128)] = jnp.concatenate(
                        [outs[2 * h], outs[2 * h + 1]], axis=0
                    ).astype(BF16)
            for xpair in range(2):
                both = [exchange_blocks([sides[1][4 * a + 2 * xpair + b] for a in range(4)]) for b in range(2)]
                for h in range(2):
                    halves = [[], []]
                    for kk in (2 * h, 2 * h + 1):
                        halves[0].append(jnp.where(near, both[0][kk], pltpu.roll(both[1][kk], 16, 1)))
                        halves[1].append(jnp.where(near, pltpu.roll(both[0][kk], 112, 1), both[1][kk]))
                    for c in range(2):
                        right[ch, c, at[h], pl.ds(xpair * 128, 128)] = jnp.concatenate(
                            halves[c], axis=0
                        ).astype(BF16)

        cross_left = pltpu.make_async_remote_copy(
            left.at[ch], left_in.at[ch], sl.at[ch], rl.at[ch], device_id=partner, device_id_type=MESH
        )
        cross_left.start()
        cross_right = pltpu.make_async_remote_copy(
            right.at[ch, 1 - core], right_in.at[ch], sr.at[ch], rr.at[ch], device_id=partner, device_id_type=MESH
        )
        cross_right.start()
        cross_left.wait()
        cross_right.wait()
        both = jnp.concatenate([right[ch, core], right_in[ch]], axis=0)
        turned = jnp.transpose(both)
        for xx in range(4):
            for v in range(4):
                at = ((xx // 2 * 4 + v) * 2 + xx % 2) * 16
                rows[xx, v * 16 : v * 16 + 16, :] = turned[at : at + 16, :]
        stacked = jnp.concatenate([left[ch], left_in[ch]], axis=0)
        for d in (2, 1, 3, 4):
            part = dot(rows[(x + d) % 4], stacked, 1, 0)
            for q in range(4):
                if d < 4:
                    xsend[ch, d - 1, q] = part[:, q * 128 : q * 128 + 128].astype(BF16)
                else:
                    own[ch, q] = part[:, q * 128 : q * 128 + 128]
            if d < 4:
                for t, q in enumerate(CHUNKS):
                    pltpu.make_async_remote_copy(
                        xsend.at[ch, d - 1, q], xrecv.at[ch, d - 1, q], sx.at[ch, d - 1, t], rx.at[ch, d - 1, t],
                        device_id=along_x(d), device_id_type=MESH,
                    ).start()

    for t, q in enumerate(CHUNKS):
        totals = []
        for ch in range(2):
            for d in range(3):
                pltpu.make_async_copy(xrecv.at[ch, d, q], xrecv.at[ch, d, q], rx.at[ch, d, t]).wait()
            total = own[ch, q]
            for d in range(3):
                total = total + xrecv[ch, d, q].astype(F32)
            totals.append(total)
        for v in range(4):
            tiles = [totals[ch][v * 16 + s * 8 : v * 16 + s * 8 + 8, :] for ch in range(2) for s in range(2)]
            for g, out in enumerate(exchange_blocks(tiles)):
                send3[q, g * 4 + v] = out.astype(BF16)

        for n in range(16):
            p = q * 16 + n

            @pl.when(p != me)
            def _(n=n, p=p):
                pltpu.make_async_remote_copy(
                    send3.at[q, n], tri.at[me], s3, r3, device_id=plane(p), device_id_type=MESH
                ).start()

    tri[me] = send3[gx // 4, me % 16]

    gain = jnp.transpose(jnp.broadcast_to(out_gain[...], (128, 128)))
    bias = jnp.transpose(jnp.broadcast_to(out_bias[...], (128, 128)))
    for ch in range(2):
        pltpu.make_async_copy(send1.at[ch, pl.ds(0, 63)], send1.at[ch, pl.ds(0, 63)], s1.at[ch]).wait()
        for d in range(3):
            for t in range(4):
                pltpu.make_async_copy(xsend.at[ch, d, t], xsend.at[ch, d, t], sx.at[ch, d, t]).wait()
    pltpu.make_async_copy(tri.at[pl.ds(0, 63)], tri.at[pl.ds(0, 63)], r3).wait()

    wide[...] = tri[...].astype(F32).reshape(512, 128)
    first = lanes((64, 128)) < 64
    pieces = []
    for m in range(4):
        one = wide[pl.ds(2 * m, 64, stride=8), :]
        two = wide[pl.ds(2 * m + 1, 64, stride=8), :]
        pieces.append(
            jnp.concatenate(
                [jnp.where(first, one, pltpu.roll(two, 64, 1)), jnp.where(first, pltpu.roll(one, 64, 1), two)], axis=0
            )
        )
    sums = jnp.concatenate(pieces, axis=1)
    off = sums - jnp.mean(sums, axis=0, keepdims=True)
    spread = jnp.mean(off * off, axis=0, keepdims=True)
    scaled = off * lax.rsqrt(spread + EPS)
    tri_normed = jnp.concatenate([scaled[:, m * 128 : m * 128 + 128] * gain + bias for m in range(4)], axis=1)
    result = dot(jnp.transpose(tri_normed.astype(BF16)), outw[...], 1, 0)
    for m in range(4):
        for r in range(2):
            for s in range(2):
                at = m * 128 + (r * 2 + s) * 32
                mixed[pl.ds(s * 8 + 2 * m + r, 32, stride=16), :] = result[at : at + 32, :]
    out_ref[...] = (gating[...] * mixed[...]).astype(BF16).reshape(32, 16, 128)
    pltpu.make_async_copy(tri.at[pl.ds(0, 63)], tri.at[pl.ds(0, 63)], s3).wait()


def on_device(pair, pair_mask, in_gain, in_bias, proj_weight, gate_weight, out_gain, out_bias, out_weight):
    vmem = pltpu.VMEM
    dma = pltpu.SemaphoreType.DMA
    args = (
        pair, pair_mask.T, in_gain.reshape(1, 128), in_bias.reshape(1, 128), proj_weight, gate_weight,
        out_gain.reshape(1, 128), out_bias.reshape(1, 128), out_weight,
    )
    args = tuple(pltpu.with_memory_space_constraint(a, pltpu.HBM) for a in args)
    return pl.pallas_call(
        kernel,
        out_shape=pltpu.VMEM((32, 16, 128), BF16),
        in_specs=[pl.BlockSpec(memory_space=pltpu.HBM)] * 9,
        out_specs=pl.BlockSpec(memory_space=pltpu.VMEM),
        scratch_shapes=[vmem(a.shape, a.dtype) for a in args]
        + [
            vmem((512, 128), F32),
            vmem((2, 512, 128), F32),
            vmem((2, 64, 8, 128), BF16),
            vmem((2, 64, 8, 128), BF16),
            vmem((2, 64, 512), BF16),
            vmem((2, 64, 512), BF16),
            vmem((2, 2, 64, 256), BF16),
            vmem((2, 64, 256), BF16),
            vmem((4, 64, 128), BF16),
            vmem((2, 3, 4, 64, 128), BF16),
            vmem((2, 3, 4, 64, 128), BF16),
            vmem((2, 4, 64, 128), F32),
            vmem((4, 16, 8, 128), BF16),
            vmem((64, 8, 128), BF16),
            vmem((512, 128), F32),
            vmem((512, 128), F32),
            vmem((512, 128), F32),
            dma((9,)), dma((2,)), dma((2,)), dma((2,)), dma((2,)), dma((2,)), dma((2,)),
            dma((2, 3, 4)), dma((2, 3, 4)), dma, dma,
        ],
        compiler_params=pltpu.CompilerParams(collective_id=1, has_side_effects=True),
    )(*args)


def solution(mesh):
    rows = P("gx", ("gy", "gz"), None)
    in_specs = (rows, P("gx", ("gy", "gz")), P(), P(), P(), P(), P(), P(), P())
    return jax.shard_map(on_device, mesh=mesh, in_specs=in_specs, out_specs=rows, check_vma=False)
```

```python
import jax
import jax.numpy as jnp
from jax import lax
from jax.experimental import pallas as pl
from jax.experimental.pallas import tpu as pltpu
from jax.sharding import PartitionSpec as P

MESH = pl.DeviceIdType.MESH
F32, BF16 = jnp.float32, jnp.bfloat16
EPS = 1e-05


def around(d):
    return min(d, 8 - d)


STEPS = sorted(
    [(a, b) for a in range(8) for b in range(8) if a or b], key=lambda s: -around(s[0]) - around(s[1])
)


def dot(a, b, ca, cb):
    return lax.dot_general(a, b, (((ca,), (cb,)), ((), ())), preferred_element_type=F32)


def lanes(shape):
    return lax.broadcasted_iota(jnp.int32, shape, 1)


def exchange_blocks(tiles):
    block = lanes(tiles[0].shape) // 32
    rolled = [[t if d == 0 else pltpu.roll(t, 32 * d, 1) for d in range(4)] for t in tiles]
    outs = []
    for b in range(4):
        out = rolled[0][(0 - b) % 4]
        for a in range(1, 4):
            out = jnp.where(block == a, rolled[a][(a - b) % 4], out)
        outs.append(out)
    return outs


def kernel(
    pair_hbm, mask_hbm, in_gain_hbm, in_bias_hbm, proj_hbm, gatew_hbm, out_gain_hbm, out_bias_hbm, outw_hbm,
    out_ref,
    pair, mask, in_gain, in_bias, proj, gatew, out_gain, out_bias, outw,
    normed, staged, send1, recv1, left, left_in, right, right_in, rows, xsend, xrecv, own, send3, tri, wide,
    gating, mixed,
    load_sem, s1, r1, sl, rl, sr, rr, sx, rx, s3, r3,
):
    gx, gy, gz = lax.axis_index("gx"), lax.axis_index("gy"), lax.axis_index("gz")
    x, core = gz // 2, gz % 2
    me = gx * 4 + gy
    partner = (gx, gy, x * 2 + 1 - core)

    y = gx // 8 * 4 + gy
    zs = [(gx + d) % 8 for d in range(8)]
    ys = [(y + d) % 8 for d in range(8)]
    tops, lows = [v // 4 * 8 for v in ys], [v % 4 for v in ys]

    def plane(p):
        return (p // 4, p % 4, gz)

    others = [(tops[b] + zs[a], lows[b]) for a, b in STEPS]

    def along_x(d):
        return (gx, gy, ((x + d) % 4) * 2 + core)

    barrier = pltpu.get_barrier_semaphore()

    for g, w in others:
        pl.semaphore_signal(barrier, inc=1, device_id=(g, w, gz), device_id_type=MESH)
    for d in range(1, 4):
        pl.semaphore_signal(barrier, inc=1, device_id=along_x(d), device_id_type=MESH)
    pl.semaphore_signal(barrier, inc=1, device_id=partner, device_id_type=MESH)

    sources = (pair_hbm, mask_hbm, in_gain_hbm, in_bias_hbm, proj_hbm, gatew_hbm, out_gain_hbm, out_bias_hbm, outw_hbm)
    places = (pair, mask, in_gain, in_bias, proj, gatew, out_gain, out_bias, outw)
    loads = [pltpu.make_async_copy(s, d, load_sem.at[n]) for n, (s, d) in enumerate(zip(sources, places))]
    for load in loads:
        load.start()
    for load in loads:
        load.wait()

    tile = pair[...].astype(F32).reshape(512, 128)
    centered = tile - jnp.mean(tile, axis=-1, keepdims=True)
    variance = jnp.mean(centered * centered, axis=-1, keepdims=True)
    scaled = centered * lax.rsqrt(variance + EPS) * in_gain[...] + in_bias[...]
    normed[...] = scaled.astype(BF16).astype(F32)
    mask_value = jnp.transpose(mask[...].astype(F32))
    masked = []
    for k in range(16):
        masked.append(normed[pl.ds(k, 32, stride=16), :] * mask_value[:, k : k + 1])
    masked = jnp.concatenate(masked, axis=0).astype(BF16)
    projected = dot(jnp.transpose(proj[...]), masked, 1, 1)
    for side in range(2):
        gate = projected[256 * side : 256 * side + 128, :]
        value = projected[256 * side + 128 : 256 * side + 256, :]
        both = jax.nn.sigmoid(gate) * value
        for ch in range(2):
            for q in range(4):
                staged[ch, pl.ds(side * 4 + q, 64, stride=8), :] = both[
                    ch * 64 : ch * 64 + 64, q * 128 : q * 128 + 128
                ]
    for ch in range(2):
        send1[ch] = staged[ch].reshape(64, 8, 128).astype(BF16)

    pl.semaphore_wait(barrier, 67)

    for ch in range(2):
        if ch == 1:

            @pl.when(core == 1)
            def _():
                pl.delay(2500)

        for g, w in others:
            pltpu.make_async_remote_copy(
                send1.at[ch, g * 4 + w], recv1.at[ch, me], s1.at[ch], r1.at[ch], device_id=(g, w, gz),
                device_id_type=MESH,
            ).start()
        recv1[ch, me] = send1[ch, me]

    gates = dot(normed[...].astype(BF16), gatew[...], 1, 0)
    gating[...] = jax.nn.sigmoid(gates)

    low = lax.broadcasted_iota(jnp.int32, (8, 128), 0) < 4
    near = lanes((8, 128)) % 32 < 16
    def partial_sums(ch, wave):
        both = jnp.concatenate([left[ch, wave], left_in[ch, wave]], axis=0)
        part = dot(rows[ch], both, 1, 0)
        for xx in range(4):
            for top in range(2):
                piece = part[xx * 64 : xx * 64 + 64, top * 128 : top * 128 + 128]
                own[ch, wave, xx, top] = piece
                xsend[ch, wave, xx, top] = piece.astype(BF16)

    def send_along_x(ch, wave, d):
        pltpu.make_async_remote_copy(
            xsend.at[ch, wave, (x + d) % 4], xrecv.at[ch, wave, d - 1], sx.at[ch, wave, d - 1], rx.at[ch, wave, d - 1],
            device_id=along_x(d), device_id_type=MESH,
        ).start()

    for ch in range(2):
        pltpu.make_async_copy(recv1.at[ch, pl.ds(0, 63)], recv1.at[ch, pl.ds(0, 63)], r1.at[ch]).wait()
        for pairing in range(2):
            at = [pl.ds(pairing * 32 + h * 16, 16) for h in range(2)]
            sides = [[], []]
            for g in range(16):
                one = recv1[ch, g * 4 + pairing * 2].astype(F32)
                two = recv1[ch, g * 4 + pairing * 2 + 1].astype(F32)
                sides[0].append(jnp.where(low, one, pltpu.roll(two, 4, 0)))
                sides[1].append(jnp.where(low, pltpu.roll(one, 4, 0), two))
            for group in range(4):
                outs = exchange_blocks([sides[0][4 * group + a] for a in range(4)])
                for h in range(2):
                    left[ch, group % 2, at[h], pl.ds(group // 2 * 128, 128)] = jnp.concatenate(
                        [outs[2 * h], outs[2 * h + 1]], axis=0
                    ).astype(BF16)
            for xpair in range(2):
                both = [exchange_blocks([sides[1][4 * a + 2 * xpair + b] for a in range(4)]) for b in range(2)]
                for h in range(2):
                    halves = [[], []]
                    for kk in (2 * h, 2 * h + 1):
                        halves[0].append(jnp.where(near, both[0][kk], pltpu.roll(both[1][kk], 16, 1)))
                        halves[1].append(jnp.where(near, pltpu.roll(both[0][kk], 112, 1), both[1][kk]))
                    for c in range(2):
                        right[ch, c, at[h], pl.ds(xpair * 128, 128)] = jnp.concatenate(
                            halves[c], axis=0
                        ).astype(BF16)

        cross_left = pltpu.make_async_remote_copy(
            left.at[ch], left_in.at[ch], sl.at[ch], rl.at[ch], device_id=partner, device_id_type=MESH
        )
        cross_left.start()
        cross_right = pltpu.make_async_remote_copy(
            right.at[ch, 1 - core], right_in.at[ch], sr.at[ch], rr.at[ch], device_id=partner, device_id_type=MESH
        )
        cross_right.start()
        if ch == 1:
            partial_sums(0, 1)
        cross_left.wait()
        cross_right.wait()
        turned = jnp.transpose(jnp.concatenate([right[ch, core], right_in[ch]], axis=0))
        for xx in range(4):
            for v in range(4):
                at = ((xx // 2 * 4 + v) * 2 + xx % 2) * 16
                rows[ch, xx * 64 + v * 16 : xx * 64 + v * 16 + 16, :] = turned[at : at + 16, :]
        partial_sums(ch, 0)
        for d in (2, 1, 3):
            send_along_x(ch, 0, d)
    partial_sums(1, 1)
    for ch in range(2):
        for d in range(3):
            pltpu.make_async_copy(xsend.at[ch, 0, d], xsend.at[ch, 0, d], sx.at[ch, 0, d]).wait()
    for ch in range(2):
        for d in (2, 1, 3):
            send_along_x(ch, 1, d)

    for wave in range(2):
        for ch in range(2):
            for d in range(3):
                pltpu.make_async_copy(xrecv.at[ch, wave, d], xrecv.at[ch, wave, d], rx.at[ch, wave, d]).wait()
        for top in range(2):
            q = top * 2 + wave
            totals = []
            for ch in range(2):
                total = own[ch, wave, x, top]
                for d in range(3):
                    total = total + xrecv[ch, wave, d, top].astype(F32)
                totals.append(total)
            for v in range(4):
                tiles = [totals[ch][v * 16 + s * 8 : v * 16 + s * 8 + 8, :] for ch in range(2) for s in range(2)]
                for g, out in enumerate(exchange_blocks(tiles)):
                    send3[q, g * 4 + v] = out.astype(BF16)

            for n in range(16):
                p = q * 16 + n

                @pl.when(p != me)
                def _(n=n, p=p, q=q):
                    pltpu.make_async_remote_copy(
                        send3.at[q, n], tri.at[me], s3, r3, device_id=plane(p), device_id_type=MESH
                    ).start()

    tri[me] = send3[gx // 4, me % 16]

    gain = jnp.transpose(jnp.broadcast_to(out_gain[...], (128, 128)))
    bias = jnp.transpose(jnp.broadcast_to(out_bias[...], (128, 128)))
    for ch in range(2):
        pltpu.make_async_copy(send1.at[ch, pl.ds(0, 63)], send1.at[ch, pl.ds(0, 63)], s1.at[ch]).wait()
        for d in range(3):
            pltpu.make_async_copy(xsend.at[ch, 1, d], xsend.at[ch, 1, d], sx.at[ch, 1, d]).wait()
    pltpu.make_async_copy(tri.at[pl.ds(0, 63)], tri.at[pl.ds(0, 63)], r3).wait()

    wide[...] = tri[...].astype(F32).reshape(512, 128)
    first = lanes((64, 128)) < 64
    pieces = []
    for m in range(4):
        one = wide[pl.ds(2 * m, 64, stride=8), :]
        two = wide[pl.ds(2 * m + 1, 64, stride=8), :]
        pieces.append(
            jnp.concatenate(
                [jnp.where(first, one, pltpu.roll(two, 64, 1)), jnp.where(first, pltpu.roll(one, 64, 1), two)], axis=0
            )
        )
    sums = jnp.concatenate(pieces, axis=1)
    off = sums - jnp.mean(sums, axis=0, keepdims=True)
    spread = jnp.mean(off * off, axis=0, keepdims=True)
    scaled = off * lax.rsqrt(spread + EPS)
    tri_normed = jnp.concatenate([scaled[:, m * 128 : m * 128 + 128] * gain + bias for m in range(4)], axis=1)
    result = dot(jnp.transpose(tri_normed.astype(BF16)), outw[...], 1, 0)
    for m in range(4):
        for r in range(2):
            for s in range(2):
                at = m * 128 + (r * 2 + s) * 32
                mixed[pl.ds(s * 8 + 2 * m + r, 32, stride=16), :] = result[at : at + 32, :]
    out_ref[...] = (gating[...] * mixed[...]).astype(BF16).reshape(32, 16, 128)
    pltpu.make_async_copy(tri.at[pl.ds(0, 63)], tri.at[pl.ds(0, 63)], s3).wait()


def on_device(pair, pair_mask, in_gain, in_bias, proj_weight, gate_weight, out_gain, out_bias, out_weight):
    vmem = pltpu.VMEM
    dma = pltpu.SemaphoreType.DMA
    args = (
        pair, pair_mask.T, in_gain.reshape(1, 128), in_bias.reshape(1, 128), proj_weight, gate_weight,
        out_gain.reshape(1, 128), out_bias.reshape(1, 128), out_weight,
    )
    args = tuple(pltpu.with_memory_space_constraint(a, pltpu.HBM) for a in args)
    return pl.pallas_call(
        kernel,
        out_shape=pltpu.VMEM((32, 16, 128), BF16),
        in_specs=[pl.BlockSpec(memory_space=pltpu.HBM)] * 9,
        out_specs=pl.BlockSpec(memory_space=pltpu.VMEM),
        scratch_shapes=[vmem(a.shape, a.dtype) for a in args]
        + [
            vmem((512, 128), F32),
            vmem((2, 512, 128), F32),
            vmem((2, 64, 8, 128), BF16),
            vmem((2, 64, 8, 128), BF16),
            vmem((2, 2, 64, 256), BF16),
            vmem((2, 2, 64, 256), BF16),
            vmem((2, 2, 64, 256), BF16),
            vmem((2, 64, 256), BF16),
            vmem((2, 256, 128), BF16),
            vmem((2, 2, 4, 2, 64, 128), BF16),
            vmem((2, 2, 3, 2, 64, 128), BF16),
            vmem((2, 2, 4, 2, 64, 128), F32),
            vmem((4, 16, 8, 128), BF16),
            vmem((64, 8, 128), BF16),
            vmem((512, 128), F32),
            vmem((512, 128), F32),
            vmem((512, 128), F32),
            dma((9,)), dma((2,)), dma((2,)), dma((2,)), dma((2,)), dma((2,)), dma((2,)),
            dma((2, 2, 3)), dma((2, 2, 3)), dma, dma,
        ],
        compiler_params=pltpu.CompilerParams(collective_id=1, has_side_effects=True),
    )(*args)


def solution(mesh):
    rows = P("gx", ("gy", "gz"), None)
    in_specs = (rows, P("gx", ("gy", "gz")), P(), P(), P(), P(), P(), P(), P())
    return jax.shard_map(on_device, mesh=mesh, in_specs=in_specs, out_specs=rows, check_vma=False)
```

```python
import jax
import jax.numpy as jnp
from jax import lax
from jax.experimental import pallas as pl
from jax.experimental.pallas import tpu as pltpu
from jax.sharding import PartitionSpec as P

MESH = pl.DeviceIdType.MESH
F32, BF16 = jnp.float32, jnp.bfloat16
EPS = 1e-05


def around(d):
    return min(d, 8 - d)


STEPS = sorted(
    [(a, b) for a in range(8) for b in range(8) if a or b], key=lambda s: -around(s[0]) - around(s[1])
)


def dot(a, b, ca, cb):
    return lax.dot_general(a, b, (((ca,), (cb,)), ((), ())), preferred_element_type=F32)


def lanes(shape):
    return lax.broadcasted_iota(jnp.int32, shape, 1)


def exchange_blocks(tiles):
    block = lanes(tiles[0].shape) // 32
    rolled = [[t if d == 0 else pltpu.roll(t, 32 * d, 1) for d in range(4)] for t in tiles]
    outs = []
    for b in range(4):
        out = rolled[0][(0 - b) % 4]
        for a in range(1, 4):
            out = jnp.where(block == a, rolled[a][(a - b) % 4], out)
        outs.append(out)
    return outs


def kernel(
    pair_hbm, mask_hbm, in_gain_hbm, in_bias_hbm, proj_hbm, gatew_hbm, out_gain_hbm, out_bias_hbm, outw_hbm,
    out_ref,
    pair, mask, in_gain, in_bias, proj, gatew, out_gain, out_bias, outw,
    normed, staged, send1, recv1, left, left_in, right, right_in, rows, xsend, xrecv, own, send3, tri, wide,
    gating, mixed,
    load_sem, s1, r1, sl, rl, sr, rr, sx, rx, s3, r3,
):
    gx, gy, gz = lax.axis_index("gx"), lax.axis_index("gy"), lax.axis_index("gz")
    x, core = gz // 2, gz % 2
    me = gx * 4 + gy
    partner = (gx, gy, x * 2 + 1 - core)

    y = gx // 8 * 4 + gy
    zs = [(gx + d) % 8 for d in range(8)]
    ys = [(y + d) % 8 for d in range(8)]
    tops, lows = [v // 4 * 8 for v in ys], [v % 4 for v in ys]

    def plane(p):
        return (p // 4, p % 4, gz)

    others = [(tops[b] + zs[a], lows[b]) for a, b in STEPS]

    def along_x(d):
        return (gx, gy, ((x + d) % 4) * 2 + core)

    barrier = pltpu.get_barrier_semaphore()

    for g, w in others:
        pl.semaphore_signal(barrier, inc=1, device_id=(g, w, gz), device_id_type=MESH)
    for d in range(1, 4):
        pl.semaphore_signal(barrier, inc=1, device_id=along_x(d), device_id_type=MESH)
    pl.semaphore_signal(barrier, inc=1, device_id=partner, device_id_type=MESH)

    sources = (pair_hbm, mask_hbm, in_gain_hbm, in_bias_hbm, proj_hbm, gatew_hbm, out_gain_hbm, out_bias_hbm, outw_hbm)
    places = (pair, mask, in_gain, in_bias, proj, gatew, out_gain, out_bias, outw)
    loads = [pltpu.make_async_copy(s, d, load_sem.at[n]) for n, (s, d) in enumerate(zip(sources, places))]
    for load in loads:
        load.start()
    for load in loads:
        load.wait()

    tile = pair[...].astype(F32).reshape(512, 128)
    centered = tile - jnp.mean(tile, axis=-1, keepdims=True)
    variance = jnp.mean(centered * centered, axis=-1, keepdims=True)
    scaled = centered * lax.rsqrt(variance + EPS) * in_gain[...] + in_bias[...]
    normed[...] = scaled.astype(BF16).astype(F32)
    mask_value = jnp.transpose(mask[...].astype(F32))
    masked = []
    for k in range(16):
        masked.append(normed[pl.ds(k, 32, stride=16), :] * mask_value[:, k : k + 1])
    masked = jnp.concatenate(masked, axis=0).astype(BF16)
    projected = dot(jnp.transpose(proj[...]), masked, 1, 1)
    for side in range(2):
        gate = projected[256 * side : 256 * side + 128, :]
        value = projected[256 * side + 128 : 256 * side + 256, :]
        both = jax.nn.sigmoid(gate) * value
        for ch in range(2):
            for q in range(4):
                staged[ch, pl.ds(side * 4 + q, 64, stride=8), :] = both[
                    ch * 64 : ch * 64 + 64, q * 128 : q * 128 + 128
                ]
    for ch in range(2):
        send1[ch] = staged[ch].reshape(64, 8, 128).astype(BF16)

    pl.semaphore_wait(barrier, 67)

    for ch in range(2):
        if ch == 1:

            @pl.when(core == 1)
            def _():
                pl.delay(2500)

        for g, w in others:
            pltpu.make_async_remote_copy(
                send1.at[ch, g * 4 + w], recv1.at[ch, me], s1.at[ch], r1.at[ch], device_id=(g, w, gz),
                device_id_type=MESH,
            ).start()
        recv1[ch, me] = send1[ch, me]

    gates = dot(normed[...].astype(BF16), gatew[...], 1, 0)
    gating[...] = jax.nn.sigmoid(gates)

    low = lax.broadcasted_iota(jnp.int32, (8, 128), 0) < 4
    near = lanes((8, 128)) % 32 < 16
    def partial_sums(ch, wave):
        both = jnp.concatenate([left[ch, wave], left_in[ch, wave]], axis=0)
        part = dot(rows[ch], both, 1, 0)
        for xx in range(4):
            for top in range(2):
                piece = part[xx * 64 : xx * 64 + 64, top * 128 : top * 128 + 128]
                own[ch, wave, xx, top] = piece
                xsend[ch, wave, xx, top] = piece.astype(BF16)

    def send_along_x(ch, wave, top):
        for d in (2, 1, 3):
            pltpu.make_async_remote_copy(
                xsend.at[ch, wave, (x + d) % 4, top], xrecv.at[ch, wave, d - 1, top], sx.at[ch, wave, top, d - 1],
                rx.at[ch, wave, top, d - 1], device_id=along_x(d), device_id_type=MESH,
            ).start()

    def sent_along_x(ch, wave, top):
        for d in range(3):
            pltpu.make_async_copy(xsend.at[ch, wave, d, top], xsend.at[ch, wave, d, top], sx.at[ch, wave, top, d]).wait()

    for ch in range(2):
        pltpu.make_async_copy(recv1.at[ch, pl.ds(0, 63)], recv1.at[ch, pl.ds(0, 63)], r1.at[ch]).wait()
        for pairing in range(2):
            at = [pl.ds(pairing * 32 + h * 16, 16) for h in range(2)]
            sides = [[], []]
            for g in range(16):
                one = recv1[ch, g * 4 + pairing * 2].astype(F32)
                two = recv1[ch, g * 4 + pairing * 2 + 1].astype(F32)
                sides[0].append(jnp.where(low, one, pltpu.roll(two, 4, 0)))
                sides[1].append(jnp.where(low, pltpu.roll(one, 4, 0), two))
            for group in range(4):
                outs = exchange_blocks([sides[0][8 * (a // 2) + 2 * group + a % 2] for a in range(4)])
                for h in range(2):
                    left[ch, group // 2, at[h], pl.ds(group % 2 * 128, 128)] = jnp.concatenate(
                        [outs[2 * h], outs[2 * h + 1]], axis=0
                    ).astype(BF16)
            for xpair in range(2):
                both = [exchange_blocks([sides[1][4 * a + 2 * xpair + b] for a in range(4)]) for b in range(2)]
                for h in range(2):
                    halves = [[], []]
                    for kk in (2 * h, 2 * h + 1):
                        halves[0].append(jnp.where(near, both[0][kk], pltpu.roll(both[1][kk], 16, 1)))
                        halves[1].append(jnp.where(near, pltpu.roll(both[0][kk], 112, 1), both[1][kk]))
                    for c in range(2):
                        right[ch, c, at[h], pl.ds(xpair * 128, 128)] = jnp.concatenate(
                            halves[c], axis=0
                        ).astype(BF16)

        cross_left = pltpu.make_async_remote_copy(
            left.at[ch], left_in.at[ch], sl.at[ch], rl.at[ch], device_id=partner, device_id_type=MESH
        )
        cross_left.start()
        cross_right = pltpu.make_async_remote_copy(
            right.at[ch, 1 - core], right_in.at[ch], sr.at[ch], rr.at[ch], device_id=partner, device_id_type=MESH
        )
        cross_right.start()
        if ch == 1:
            partial_sums(0, 1)
        cross_left.wait()
        cross_right.wait()
        turned = jnp.transpose(jnp.concatenate([right[ch, core], right_in[ch]], axis=0))
        for xx in range(4):
            for v in range(4):
                at = ((xx // 2 * 4 + v) * 2 + xx % 2) * 16
                rows[ch, xx * 64 + v * 16 : xx * 64 + v * 16 + 16, :] = turned[at : at + 16, :]
        partial_sums(ch, 0)
        send_along_x(ch, 0, 0)
        if ch == 0:
            send_along_x(0, 0, 1)
    partial_sums(1, 1)
    sent_along_x(0, 0, 0)
    sent_along_x(0, 0, 1)
    sent_along_x(1, 0, 0)
    send_along_x(1, 0, 1)
    sent_along_x(1, 0, 1)
    for top in range(2):
        for ch in range(2):
            send_along_x(ch, 1, top)

    for wave in range(2):
        for top in range(2):
            for ch in range(2):
                for d in range(3):
                    arrived = xrecv.at[ch, wave, d, top]
                    pltpu.make_async_copy(arrived, arrived, rx.at[ch, wave, top, d]).wait()
            totals = []
            for ch in range(2):
                total = own[ch, wave, x, top]
                for d in range(3):
                    total = total + xrecv[ch, wave, d, top].astype(F32)
                totals.append(total)
            for v in range(4):
                tiles = [totals[ch][v * 16 + s * 8 : v * 16 + s * 8 + 8, :] for ch in range(2) for s in range(2)]
                for g, out in enumerate(exchange_blocks(tiles)):
                    p = (g // 2 * 8 + wave * 4 + top * 2 + g % 2) * 4 + v
                    send3[p] = out.astype(BF16)
                for g in range(4):
                    p = (g // 2 * 8 + wave * 4 + top * 2 + g % 2) * 4 + v

                    @pl.when(me != p)
                    def _(p=p):
                        pltpu.make_async_remote_copy(
                            send3.at[p], tri.at[me], s3, r3, device_id=plane(p), device_id_type=MESH
                        ).start()

    tri[me] = send3[me]

    gain = jnp.transpose(jnp.broadcast_to(out_gain[...], (128, 128)))
    bias = jnp.transpose(jnp.broadcast_to(out_bias[...], (128, 128)))
    for ch in range(2):
        pltpu.make_async_copy(send1.at[ch, pl.ds(0, 63)], send1.at[ch, pl.ds(0, 63)], s1.at[ch]).wait()
        for top in range(2):
            sent_along_x(ch, 1, top)
    pltpu.make_async_copy(tri.at[pl.ds(0, 63)], tri.at[pl.ds(0, 63)], r3).wait()

    wide[...] = tri[...].astype(F32).reshape(512, 128)
    first = lanes((64, 128)) < 64
    pieces = []
    for m in range(4):
        one = wide[pl.ds(2 * m, 64, stride=8), :]
        two = wide[pl.ds(2 * m + 1, 64, stride=8), :]
        pieces.append(
            jnp.concatenate(
                [jnp.where(first, one, pltpu.roll(two, 64, 1)), jnp.where(first, pltpu.roll(one, 64, 1), two)], axis=0
            )
        )
    sums = jnp.concatenate(pieces, axis=1)
    off = sums - jnp.mean(sums, axis=0, keepdims=True)
    spread = jnp.mean(off * off, axis=0, keepdims=True)
    scaled = off * lax.rsqrt(spread + EPS)
    tri_normed = jnp.concatenate([scaled[:, m * 128 : m * 128 + 128] * gain + bias for m in range(4)], axis=1)
    result = dot(jnp.transpose(tri_normed.astype(BF16)), outw[...], 1, 0)
    for m in range(4):
        for r in range(2):
            for s in range(2):
                at = m * 128 + (r * 2 + s) * 32
                mixed[pl.ds(s * 8 + 2 * m + r, 32, stride=16), :] = result[at : at + 32, :]
    out_ref[...] = (gating[...] * mixed[...]).astype(BF16).reshape(32, 16, 128)
    pltpu.make_async_copy(tri.at[pl.ds(0, 63)], tri.at[pl.ds(0, 63)], s3).wait()


def on_device(pair, pair_mask, in_gain, in_bias, proj_weight, gate_weight, out_gain, out_bias, out_weight):
    vmem = pltpu.VMEM
    dma = pltpu.SemaphoreType.DMA
    args = (
        pair, pair_mask.T, in_gain.reshape(1, 128), in_bias.reshape(1, 128), proj_weight, gate_weight,
        out_gain.reshape(1, 128), out_bias.reshape(1, 128), out_weight,
    )
    args = tuple(pltpu.with_memory_space_constraint(a, pltpu.HBM) for a in args)
    return pl.pallas_call(
        kernel,
        out_shape=pltpu.VMEM((32, 16, 128), BF16),
        in_specs=[pl.BlockSpec(memory_space=pltpu.HBM)] * 9,
        out_specs=pl.BlockSpec(memory_space=pltpu.VMEM),
        scratch_shapes=[vmem(a.shape, a.dtype) for a in args]
        + [
            vmem((512, 128), F32),
            vmem((2, 512, 128), F32),
            vmem((2, 64, 8, 128), BF16),
            vmem((2, 64, 8, 128), BF16),
            vmem((2, 2, 64, 256), BF16),
            vmem((2, 2, 64, 256), BF16),
            vmem((2, 2, 64, 256), BF16),
            vmem((2, 64, 256), BF16),
            vmem((2, 256, 128), BF16),
            vmem((2, 2, 4, 2, 64, 128), BF16),
            vmem((2, 2, 3, 2, 64, 128), BF16),
            vmem((2, 2, 4, 2, 64, 128), F32),
            vmem((64, 8, 128), BF16),
            vmem((64, 8, 128), BF16),
            vmem((512, 128), F32),
            vmem((512, 128), F32),
            vmem((512, 128), F32),
            dma((9,)), dma((2,)), dma((2,)), dma((2,)), dma((2,)), dma((2,)), dma((2,)),
            dma((2, 2, 2, 3)), dma((2, 2, 2, 3)), dma, dma,
        ],
        compiler_params=pltpu.CompilerParams(collective_id=1, has_side_effects=True),
    )(*args)


def solution(mesh):
    rows = P("gx", ("gy", "gz"), None)
    in_specs = (rows, P("gx", ("gy", "gz")), P(), P(), P(), P(), P(), P(), P())
    return jax.shard_map(on_device, mesh=mesh, in_specs=in_specs, out_specs=rows, check_vma=False)
```
